32 devices in a mesh: section: 2 (over x), mp: 8 (over z, core), req: 2 (over y).
Axes of the slice: x: 2, y: 2, z: 4, core: 2. Of those that a mesh axis runs over, the one named last changes fastest.
Arguments:
- tokens: bfloat16 [256, 4, 4096], P('mp', 'req'), may hold values from -6 to 6
- lengths: int32 [4], replicated, may hold values from 32 to 256
- assign: int32 [4], replicated, may hold values from 0 to 3, as said below
- w_qkv: bfloat16 [2, 4096, 3, 4096], P('section', None, None, 'mp'), may hold values from -0.09375 to 0.09375
- w_out: bfloat16 [2, 4096, 4096], P('section', 'mp'), may hold values from -0.09375 to 0.09375
- w_in: bfloat16 [2, 4096, 2, 10240], P('section', None, None, 'mp'), may hold values from -0.09375 to 0.09375
- w_down: bfloat16 [2, 10240, 4096], P('section', 'mp'), may hold values from -0.0625 to 0.0625
- enc_gains: bfloat16 [2, 2, 4096], P('section'), may hold values from 0.5 to 1.5
- final_gain: bfloat16 [4096], replicated, may hold values from 0.5 to 1.5
- w_memory: bfloat16 [4096, 2, 4096], P(None, None, 'mp'), may hold values from -0.09375 to 0.09375
- dec_input: bfloat16 [4, 4096], replicated, may hold values from -6 to 6
- dec_gain: bfloat16 [4096], replicated, may hold values from 0.29882812 to 3
- w_query: bfloat16 [4096, 4096], P(None, 'mp'), may hold values from -0.09375 to 0.09375
- w_cross_out: bfloat16 [4096, 4096], P('mp'), may hold values from -0.09375 to 0.09375
Outputs:
- memory_kv: bfloat16 [4, 256, 2, 4096], P(('section', 'req'), None, None, 'mp')
- dec_output: bfloat16 [4, 4096], P(('section', 'req'))
The draws below stay inside these ranges and needn't reach their ends.
Inputs may be any that keep to these rules, and one draw needn't show every extreme that they name: `assign`: each of the 4 decode groups is named by exactly 1 request.
All inputs are finite; a program needn't handle non-finite values.
Results may differ from the reference program's by a relative error of at most 0.035.
Values may be sent and summed in bfloat16 or wider, within the bound.
No kernel may reach another device: no remote copies, remote signals or barrier semaphores. Data moves between devices by JAX's collectives and lax.ppermute only.
A program may use at most 128 MiB of HBM per device.

```python
import math
import jax
import jax.numpy as jnp
from jax import lax

D = 4096
HEADS = 64
HD = 64
FF = 10240
LEN = 256
LAYERS = 2
REQUESTS = 4
GROUPS = 4
PER_GROUP = 1
N_MP = 8


def draw_assign(key, part):
    return (jax.random.permutation(key, REQUESTS) // PER_GROUP).astype(jnp.int32)


def set_ends(values, key, low, high):
    shape = values.shape
    index_at = [jax.random.randint(jax.random.fold_in(key, axis), (), 0, shape[axis]) for axis in range(len(shape))]
    values = values.at[tuple(index_at)].set(low)
    longest = shape.index(max(shape))
    index_at[longest] = (index_at[longest] + 1) % shape[longest]
    return values.at[tuple(index_at)].set(high)


def levels(key, dims, cuts, smallest, high):
    factor_of, own = 1.0, jax.random.fold_in(key, 6)
    for axis_at, blocks in cuts:
        steps = jnp.exp(jax.random.uniform(jax.random.fold_in(own, axis_at), (blocks,), jnp.float32, smallest / len(cuts), high / len(cuts)))
        factor_of = factor_of * jnp.repeat(steps, dims[axis_at] // blocks).reshape([-1 if axis == axis_at else 1 for axis in range(len(dims))])
    return factor_of


def gaussian(stream_key, extent, spread, reach, pieces=(), kind=jnp.bfloat16):
    array = jax.random.normal(stream_key, extent, jnp.float32) * spread
    if len(pieces) > 0:
        array = levels(stream_key, extent, pieces, -0.22, 0.18) * array
    return jnp.clip(array, min=-reach, max=reach).astype(kind)


def setup_inputs(seed: int = 0) -> dict:
    key_list = jax.random.split(jax.random.key(seed), 15)
    tokens = gaussian(key_list[0], (LEN, REQUESTS, D), 1.0, 6.0, ((0, 8), (1, 2)))
    lengths = set_ends(jax.random.randint(key_list[1], (REQUESTS,), LEN // 8, LEN + 1), jax.random.fold_in(key_list[1], 1), LEN // 8, LEN).astype(jnp.int32)
    assign = draw_assign(jax.random.fold_in(key_list[14], 71), 0)
    w_qkv = gaussian(key_list[3], (LAYERS, D, 3, HEADS * HD), D ** -0.5, 0.09375, ((0, 2), (3, 8)))
    w_out = gaussian(key_list[4], (LAYERS, HEADS * HD, D), (HEADS * HD) ** -0.5, 0.09375, ((0, 2), (1, 8)))
    w_in = gaussian(key_list[5], (LAYERS, D, 2, FF), D ** -0.5, 0.09375, ((0, 2), (3, 8)))
    w_down = gaussian(key_list[6], (LAYERS, FF, D), FF ** -0.5, 0.0625, ((0, 2), (1, 8)))
    enc_gains = jnp.clip(1.0 + 0.1 * jax.random.normal(key_list[7], (LAYERS, 2, D), jnp.float32), 0.5, 1.5).astype(jnp.bfloat16)
    final_gain = jnp.clip(1.0 + 0.1 * jax.random.normal(key_list[8], (D,), jnp.float32), 0.5, 1.5).astype(jnp.bfloat16)
    w_memory = gaussian(key_list[9], (D, 2, HEADS * HD), D ** -0.5, 0.09375, ((2, 8),))
    dec_input = gaussian(key_list[10], (REQUESTS, D), 1.0, 6.0)
    dec_gain = jnp.clip(jnp.exp(jax.random.uniform(key_list[11], (D,), jnp.float32, math.log(0.29882812), math.log(3.0))), 0.29882812, 3.0).astype(jnp.bfloat16)
    w_query = gaussian(key_list[12], (D, HEADS * HD), D ** -0.5, 0.09375, ((1, 8),))
    w_cross_out = gaussian(key_list[13], (HEADS * HD, D), (HEADS * HD) ** -0.5, 0.09375, ((0, 8),))
    return dict(tokens=tokens, lengths=lengths, assign=assign, w_qkv=w_qkv, w_out=w_out, w_in=w_in, w_down=w_down, enc_gains=enc_gains, final_gain=final_gain, w_memory=w_memory, dec_input=dec_input, dec_gain=dec_gain, w_query=w_query, w_cross_out=w_cross_out)


EPSILON = 1e-06

def rms_norm(values, gain):
    return values * lax.rsqrt(lax.optimization_barrier(jnp.mean(values * values, axis=-1, keepdims=True)) + EPSILON) * gain.astype(jnp.float32)

def shard_total(active, weight):
    length, batch, inner = active.shape
    split = active.astype(jnp.float32).reshape(length, batch, N_MP, inner // N_MP)
    blocks = weight.astype(jnp.float32).reshape(N_MP, inner // N_MP, weight.shape[1])
    partial_sums = jnp.einsum('lbnk,nkd->lbnd', split, blocks)
    rounded = lax.optimization_barrier(partial_sums.astype(jnp.bfloat16))
    return lax.optimization_barrier(jnp.sum(rounded.astype(jnp.float32), axis=2))

def self_attend(query, keys, values, valid):
    scores = jnp.einsum('qbhe,kbhe->bhqk', query.astype(jnp.float32), keys.astype(jnp.float32)) * HD ** (-0.5)
    scores = jnp.where(valid[:, None, None, :], scores, -1000000000.0)
    weights = jax.nn.softmax(scores, axis=-1).astype(jnp.bfloat16)
    context = jnp.einsum('bhqk,kbhe->qbhe', weights.astype(jnp.float32), values.astype(jnp.float32))
    return context.astype(jnp.bfloat16)

def encoder_layer(hidden_in, valid, weight_qkv, weight_out, weight_in, weight_down, gains):
    length, batch, _ = hidden_in.shape
    stream = hidden_in.astype(jnp.float32)
    normed = rms_norm(stream, gains[0]).astype(jnp.bfloat16)
    projected = jnp.einsum('lbd,dce->lbce', normed.astype(jnp.float32), weight_qkv.astype(jnp.float32)).astype(jnp.bfloat16)
    split_heads = projected.reshape(length, batch, 3, HEADS, HD)
    context = self_attend(split_heads[:, :, 0], split_heads[:, :, 1], split_heads[:, :, 2], valid)
    stream = stream + shard_total(context.reshape(length, batch, HEADS * HD), weight_out)
    normed = rms_norm(stream, gains[1]).astype(jnp.bfloat16)
    gate_up = jnp.einsum('lbd,dcf->lbcf', normed.astype(jnp.float32), weight_in.astype(jnp.float32))
    inner = (jax.nn.gelu(gate_up[:, :, 0], approximate=True) * gate_up[:, :, 1]).astype(jnp.bfloat16)
    stream = stream + shard_total(inner, weight_down)
    return stream.astype(jnp.bfloat16)

def destinations(assign, per_group):
    count = assign.shape[0]
    order = jnp.arange(count, dtype=jnp.int32)
    same = assign[None, :] == assign[:, None]
    earlier = order[None, :] < order[:, None]
    slots = lax.optimization_barrier(jnp.sum((same & earlier).astype(jnp.int32), axis=1))
    return assign * per_group + slots

def reference(tokens, lengths, assign, w_qkv, w_out, w_in, w_down, enc_gains, final_gain, w_memory, dec_input, dec_gain, w_query, w_cross_out):
    positions = jnp.arange(LEN, dtype=jnp.int32)
    valid = positions[None, :] < lengths[:, None]
    hidden = tokens
    for layer in range(LAYERS):
        hidden = encoder_layer(hidden, valid, w_qkv[layer], w_out[layer], w_in[layer], w_down[layer], enc_gains[layer])
    normed = rms_norm(hidden.astype(jnp.float32), final_gain).astype(jnp.bfloat16)
    memory_rows = jnp.einsum('lbd,dce->lbce', normed.astype(jnp.float32), w_memory.astype(jnp.float32)).astype(jnp.bfloat16)
    target = destinations(assign, PER_GROUP)
    slot_ids = jnp.arange(GROUPS * PER_GROUP, dtype=jnp.int32)
    picker = (target[None, :] == slot_ids[:, None]).astype(jnp.float32)
    memory_kv = jnp.einsum('ob,lbce->olce', picker, memory_rows.astype(jnp.float32)).astype(jnp.bfloat16)
    query_rows = jnp.dot(picker, dec_input.astype(jnp.float32), precision=lax.Precision.HIGHEST)
    query_lengths = lax.optimization_barrier(jnp.sum(jnp.where(picker > 0.5, lengths[None, :], 0), axis=1))
    slots = GROUPS * PER_GROUP
    dec_normed = rms_norm(query_rows, dec_gain).astype(jnp.bfloat16)
    query = jnp.dot(dec_normed, w_query, preferred_element_type=jnp.float32).astype(jnp.bfloat16).reshape(slots, HEADS, HD)
    cross_keys = memory_kv[:, :, 0].reshape(slots, LEN, HEADS, HD)
    cross_values = memory_kv[:, :, 1].reshape(slots, LEN, HEADS, HD)
    scores = jnp.einsum('ohe,olhe->ohl', query.astype(jnp.float32), cross_keys.astype(jnp.float32)) * HD ** (-0.5)
    scores = jnp.where(positions[None, None, :] < query_lengths[:, None, None], scores, -1000000000.0)
    weights = jax.nn.softmax(scores, axis=-1).astype(jnp.bfloat16)
    context = jnp.einsum('ohl,olhe->ohe', weights.astype(jnp.float32), cross_values.astype(jnp.float32)).astype(jnp.bfloat16)
    dec_output = (query_rows + jnp.dot(context.reshape(slots, HEADS * HD), w_cross_out, preferred_element_type=jnp.float32)).astype(jnp.bfloat16)
    return (memory_kv, dec_output)
```

```python
import jax
import jax.numpy as jnp
from jax import lax
from jax.experimental import pallas as pl
from jax.sharding import PartitionSpec as P

HD = 64

EPSILON = 1e-06


def rms_norm(values, gain):
    return (
        values
        * lax.rsqrt(jnp.mean(values * values, axis=-1, keepdims=True) + EPSILON)
        * gain.astype(jnp.float32)
    )


def columns_of(count, most):
    for size in (512, 256, 128):
        if size <= most and count % size == 0:
            return size
    return count


def plane_products(rows, planes, most=256):
    m, k = rows.shape
    p, _, n = planes.shape
    step = columns_of(n, most)

    def body(rows_ref, plane_ref, out_ref):
        out_ref[0] = jnp.dot(
            rows_ref[...], plane_ref[0], preferred_element_type=jnp.float32
        ).astype(jnp.bfloat16)

    return pl.pallas_call(
        body,
        grid=(p, n // step),
        in_specs=[
            pl.BlockSpec((m, k), lambda i, j: (0, 0)),
            pl.BlockSpec((1, k, step), lambda i, j: (i, 0, j)),
        ],
        out_specs=pl.BlockSpec((1, m, step), lambda i, j: (i, 0, j)),
        out_shape=jax.ShapeDtypeStruct((p, m, n), jnp.bfloat16),
        cost_estimate=pl.CostEstimate(
            flops=2 * m * k * n * p,
            bytes_accessed=2 * (m * k + p * k * n + p * m * n),
            transcendentals=0,
        ),
        name="plane_products",
    )(rows, planes)


def gated_products(rows, planes, most=256):
    m, k = rows.shape
    _, _, n = planes.shape
    step = columns_of(n, most)

    def body(rows_ref, plane_ref, out_ref):
        gate = jnp.dot(rows_ref[...], plane_ref[0], preferred_element_type=jnp.float32)
        up = jnp.dot(rows_ref[...], plane_ref[1], preferred_element_type=jnp.float32)
        out_ref[...] = (jax.nn.gelu(gate, approximate=True) * up).astype(jnp.bfloat16)

    return pl.pallas_call(
        body,
        grid=(n // step,),
        in_specs=[
            pl.BlockSpec((m, k), lambda j: (0, 0)),
            pl.BlockSpec((2, k, step), lambda j: (0, 0, j)),
        ],
        out_specs=pl.BlockSpec((m, step), lambda j: (0, j)),
        out_shape=jax.ShapeDtypeStruct((m, n), jnp.bfloat16),
        cost_estimate=pl.CostEstimate(
            flops=4 * m * k * n,
            bytes_accessed=2 * (m * k + 2 * k * n + m * n),
            transcendentals=m * n,
        ),
        name="gated_products",
    )(rows, planes)


def gather_rows(rows, direct):
    count = lax.axis_size("mp")
    n, width = rows.shape
    if not direct:
        whole = lax.all_gather(rows, "mp", axis=0, tiled=True)
        return whole, None
    me = lax.axis_index("mp")
    chips = count // 2
    mates = [(i, i ^ 1) for i in range(count)]
    blocks = [rows]
    owners = [me]
    hops = sorted(range(1, chips), key=lambda k: -min(k, chips - k))
    for k in hops:
        pairs = [(i, (i + 2 * k) % count) for i in range(count)]
        blocks.append(lax.ppermute(rows, "mp", pairs))
        owners.append((me - 2 * k) % count)
    blocks = blocks + [lax.ppermute(block, "mp", mates) for block in blocks]
    owners = owners + [owner ^ 1 for owner in owners]
    return jnp.concatenate(blocks, axis=0), jnp.stack(owners)


def relay_gather(rows, relay, home, other):
    count = lax.axis_size("mp")
    chips = count // 2
    both = ("section", "mp")
    me = lax.axis_index("mp")
    half = rows.shape[1] // 2

    def pairs(source, hops):
        return [
            (source * count + 2 * a + c, home * count + 2 * b + c)
            for a, b in hops
            for c in range(2)
        ]

    across = [(z, (z + 2) % chips) for z in range(chips)]
    ends = [(0, chips - 1), (chips - 1, 0)]
    up = [(z, z + 1) for z in range(chips - 1)]
    down = [(z + 1, z) for z in range(chips - 1)]
    mates = [(i, i ^ 1) for i in range(count)]
    near_half = lax.ppermute(rows[:, :half], both, pairs(home, across))
    wrapped = lax.ppermute(relay, both, pairs(other, ends))
    far_half = lax.ppermute(relay[:, half:], both, pairs(other, across))
    below = lax.ppermute(rows, both, pairs(home, up))
    above = lax.ppermute(rows, both, pairs(home, down))
    chip = me // 2
    below = jnp.where(chip == 0, wrapped, below)
    above = jnp.where(chip == chips - 1, wrapped, above)
    blocks = [rows, near_half, far_half, below, above]
    blocks = blocks + [lax.ppermute(block, "mp", mates) for block in blocks]
    owners = [me, (me - 4) % count, (me - 2) % count, (me + 2) % count]
    owners = owners + [owner ^ 1 for owner in owners]
    return jnp.concatenate(blocks, axis=1), jnp.stack(owners)


def row_positions(owners, length):
    local = jnp.arange(length, dtype=jnp.int32)
    if owners is None:
        return local
    rows_each = length // owners.shape[0]
    return (owners[:, None] * rows_each + local[None, :rows_each]).reshape(-1)


def move_rows(values, places):
    source = jnp.arange(values.shape[0], dtype=jnp.int32)
    pick = (source[:, None] == places[None, :]).astype(values.dtype)
    moved = jnp.dot(pick, values, preferred_element_type=jnp.float32)
    return moved.astype(values.dtype)


def attention_part(whole, owners, key_lengths, weight_qkv, weight_out):
    count = lax.axis_size("mp")
    requests, length, width = whole.shape
    local_cols = weight_qkv.shape[2]
    heads = local_cols // HD
    parts = plane_products(
        whole.reshape(requests * length, width), weight_qkv.transpose(1, 0, 2)
    ).reshape(3, requests, length, heads, HD)
    positions = row_positions(owners, length)
    valid = positions[None, :] < key_lengths[:, None]
    scores = jnp.einsum(
        "bqhe,bkhe->bhqk", parts[0], parts[1], preferred_element_type=jnp.float32
    ) * HD ** (-0.5)
    scores = jnp.where(valid[:, None, None, :], scores, -1000000000.0)
    probs = jax.nn.softmax(scores, axis=-1).astype(jnp.bfloat16)
    context = jnp.einsum("bhqk,bkhe->bqhe", probs, parts[2], preferred_element_type=jnp.float32)
    context = context.astype(jnp.bfloat16).reshape(requests * length, local_cols)
    each = length // count
    request = jnp.arange(requests, dtype=jnp.int32)[:, None]
    places = (positions // each)[None, :] * (requests * each) + request * each + positions % each
    context = move_rows(context, places.reshape(-1))
    partial_out = plane_products(context, weight_out[None], 512)[0]
    return lax.psum_scatter(partial_out, "mp", scatter_dimension=0, tiled=True)


def forward_part(whole, weight_in, weight_down):
    inner = gated_products(whole, weight_in.transpose(1, 0, 2))
    partial_out = plane_products(inner, weight_down[None], 512)[0]
    return lax.psum_scatter(partial_out, "mp", scatter_dimension=0, tiled=True)


def destinations(assign, per_group):
    count = assign.shape[0]
    order = jnp.arange(count, dtype=jnp.int32)
    same = assign[None, :] == assign[:, None]
    earlier = order[None, :] < order[:, None]
    slots = jnp.sum((same & earlier).astype(jnp.int32), axis=1)
    return assign * per_group + slots


def sum_over_mp(values):
    count = lax.axis_size("mp")
    step = 1
    while step < count:
        values = values + lax.ppermute(values, "mp", [(i, i ^ step) for i in range(count)])
        step *= 2
    return values


def per_device(
    tokens,
    lengths,
    assign,
    w_qkv,
    w_out,
    w_in,
    w_down,
    enc_gains,
    final_gain,
    w_memory,
    dec_input,
    dec_gain,
    w_query,
    w_cross_out,
):
    sections = lax.axis_size("section")
    section_id = lax.axis_index("section")
    req_count = lax.axis_size("req")
    req_id = lax.axis_index("req")
    mp_count = lax.axis_size("mp")
    local_rows, group_requests, width = tokens.shape
    full_length = local_rows * mp_count
    direct = mp_count // 2 <= 4
    relayed = mp_count // 2 == 4 and sections > 1

    groups = sections * req_count
    per_group = lengths.shape[0] // groups
    target = destinations(assign, per_group)
    mine = lax.dynamic_slice_in_dim(target, req_id * group_requests, group_requests)
    slot_ids = jnp.arange(groups * per_group, dtype=jnp.int32)
    group_id = section_id * req_count + req_id
    picker_all = (target[None, :] == slot_ids[:, None]).astype(jnp.float32)
    picker = lax.dynamic_slice_in_dim(picker_all, group_id * per_group, per_group, 0)
    query_rows = jnp.dot(picker, dec_input.astype(jnp.float32), precision=lax.Precision.HIGHEST)
    query_lengths = jnp.sum(jnp.where(picker > 0.5, lengths[None, :], 0), axis=1)
    dec_normed = rms_norm(query_rows, dec_gain).astype(jnp.bfloat16)
    local_cols = w_query.shape[1]
    local_heads = local_cols // HD
    query = (
        jnp.dot(dec_normed, w_query, preferred_element_type=jnp.float32)
        .astype(jnp.bfloat16)
        .reshape(per_group, local_heads, HD)
    )

    key_lengths = lax.dynamic_slice_in_dim(lengths, req_id * group_requests, group_requests)
    gain = enc_gains[0, 0]
    flat = (group_requests * local_rows, width)

    def norm_rows(values, by):
        return rms_norm(values.astype(jnp.float32), by).astype(jnp.bfloat16)

    hidden = tokens.transpose(1, 0, 2)
    for layer in range(sections):
        other = layer - 1 if layer > 0 else 1
        if relayed:
            relay = norm_rows(hidden, lax.ppermute(gain, "section", [(layer, other)]))
        if layer > 0:
            hidden = lax.ppermute(hidden, "section", [(layer - 1, layer)])
        normed = norm_rows(hidden, gain)
        if relayed:
            whole, owners = relay_gather(normed, relay, layer, other)
        else:
            whole, owners = lax.all_gather(normed, "mp", axis=1, tiled=True), None
        part = attention_part(whole, owners, key_lengths, w_qkv[0], w_out[0])
        stream = hidden.astype(jnp.float32) + part.astype(jnp.float32).reshape(hidden.shape)
        normed = norm_rows(stream, enc_gains[0, 1]).reshape(flat)
        part = forward_part(
            lax.all_gather(normed, "mp", axis=0, tiled=True), w_in[0], w_down[0]
        )
        if layer == sections - 1:
            memory_planes = w_memory.transpose(1, 0, 2)
            part, memory_planes = lax.optimization_barrier((part, memory_planes))
        stream = stream + part.astype(jnp.float32).reshape(stream.shape)
        hidden = stream.astype(jnp.bfloat16)

    last = rms_norm(hidden.astype(jnp.float32), final_gain).astype(jnp.bfloat16)
    normed = [last[j] for j in range(group_requests)]
    chosen = mine[None, :] == slot_ids[:, None]
    outgoing = sum(
        jnp.where(chosen[:, r, None, None], normed[r][None], jnp.bfloat16(0))
        for r in range(group_requests)
    )
    incoming = lax.all_to_all(outgoing, ("section", "req"), split_axis=0, concat_axis=0, tiled=True)
    incoming = incoming.reshape(sections, req_count, per_group, local_rows, width)[sections - 1]
    received = incoming[0]
    for source in range(1, req_count):
        received = received + incoming[source]
    gathered, owners = gather_rows(
        received.transpose(1, 0, 2).reshape(local_rows * per_group, width), direct
    )
    columns = plane_products(gathered, memory_planes)
    columns = columns.transpose(1, 0, 2).reshape(full_length * per_group, 2 * local_cols)
    if owners is not None:
        block = local_rows * per_group
        inside = jnp.arange(block, dtype=jnp.int32)
        columns = move_rows(columns, (owners[:, None] * block + inside[None, :]).reshape(-1))
    columns = columns.reshape(full_length, per_group, 2, local_cols)
    memory_kv = columns.transpose(1, 0, 2, 3)
    columns = [columns[:, :, 0], columns[:, :, 1]]
    cross_keys = columns[0].reshape(full_length, per_group, local_heads, HD)
    cross_values = columns[1].reshape(full_length, per_group, local_heads, HD)
    positions = jnp.arange(full_length, dtype=jnp.int32)
    scores = jnp.einsum(
        "ohe,lohe->ohl", query, cross_keys, preferred_element_type=jnp.float32
    ) * HD ** (-0.5)
    scores = jnp.where(
        positions[None, None, :] < query_lengths[:, None, None], scores, -1000000000.0
    )
    weights = jax.nn.softmax(scores, axis=-1).astype(jnp.bfloat16)
    context = jnp.einsum(
        "ohl,lohe->ohe", weights, cross_values, preferred_element_type=jnp.float32
    ).astype(jnp.bfloat16)
    partial_out = jnp.dot(
        context.reshape(per_group, local_cols), w_cross_out, preferred_element_type=jnp.float32
    )
    total_out = sum_over_mp(partial_out)
    dec_output = (query_rows + total_out).astype(jnp.bfloat16)
    return (memory_kv, dec_output)


def solution(mesh):
    return jax.shard_map(
        per_device,
        mesh=mesh,
        in_specs=(
            P("mp", "req", None),
            P(),
            P(),
            P("section", None, None, "mp"),
            P("section", "mp", None),
            P("section", None, None, "mp"),
            P("section", "mp", None),
            P("section", None, None),
            P(),
            P(None, None, "mp"),
            P(),
            P(),
            P(None, "mp"),
            P("mp", None),
        ),
        out_specs=(P(("section", "req"), None, None, "mp"), P(("section", "req"), None)),
        check_vma=False,
    )
```

```python
import jax
import jax.numpy as jnp
from jax import lax
from jax.experimental import pallas as pl
from jax.sharding import PartitionSpec as P

HD = 64

EPSILON = 1e-06


def rms_norm(values, gain):
    return (
        values
        * lax.rsqrt(jnp.mean(values * values, axis=-1, keepdims=True) + EPSILON)
        * gain.astype(jnp.float32)
    )


def columns_of(count, most):
    for size in (1024, 512, 256, 128):
        if size <= most and count % size == 0:
            return size
    return count


def plane_products(rows, planes, most=512):
    m, k = rows.shape
    p, _, n = planes.shape
    step = columns_of(n, most)

    def body(rows_ref, plane_ref, out_ref):
        out_ref[0] = jnp.dot(
            rows_ref[...], plane_ref[0], preferred_element_type=jnp.float32
        ).astype(jnp.bfloat16)

    return pl.pallas_call(
        body,
        grid=(p, n // step),
        in_specs=[
            pl.BlockSpec((m, k), lambda i, j: (0, 0)),
            pl.BlockSpec((1, k, step), lambda i, j: (i, 0, j)),
        ],
        out_specs=pl.BlockSpec((1, m, step), lambda i, j: (i, 0, j)),
        out_shape=jax.ShapeDtypeStruct((p, m, n), jnp.bfloat16),
        cost_estimate=pl.CostEstimate(
            flops=2 * m * k * n * p,
            bytes_accessed=2 * (m * k + p * k * n + p * m * n),
            transcendentals=0,
        ),
        name="plane_products",
    )(rows, planes)


def gated_products(rows, planes, most=256):
    m, k = rows.shape
    _, _, n = planes.shape
    step = columns_of(n, most)

    def body(rows_ref, plane_ref, out_ref):
        gate = jnp.dot(rows_ref[...], plane_ref[0], preferred_element_type=jnp.float32)
        up = jnp.dot(rows_ref[...], plane_ref[1], preferred_element_type=jnp.float32)
        out_ref[...] = (jax.nn.gelu(gate, approximate=True) * up).astype(jnp.bfloat16)

    return pl.pallas_call(
        body,
        grid=(n // step,),
        in_specs=[
            pl.BlockSpec((m, k), lambda j: (0, 0)),
            pl.BlockSpec((2, k, step), lambda j: (0, 0, j)),
        ],
        out_specs=pl.BlockSpec((m, step), lambda j: (0, j)),
        out_shape=jax.ShapeDtypeStruct((m, n), jnp.bfloat16),
        cost_estimate=pl.CostEstimate(
            flops=4 * m * k * n,
            bytes_accessed=2 * (m * k + 2 * k * n + m * n),
            transcendentals=m * n,
        ),
        name="gated_products",
    )(rows, planes)


def gather_rows(rows, direct):
    count = lax.axis_size("mp")
    n, width = rows.shape
    if not direct:
        whole = lax.all_gather(rows, "mp", axis=0, tiled=True)
        return whole, None
    me = lax.axis_index("mp")
    chips = count // 2
    mates = [(i, i ^ 1) for i in range(count)]
    blocks = [rows]
    owners = [me]
    hops = sorted(range(1, chips), key=lambda k: -min(k, chips - k))
    for k in hops:
        pairs = [(i, (i + 2 * k) % count) for i in range(count)]
        blocks.append(lax.ppermute(rows, "mp", pairs))
        owners.append((me - 2 * k) % count)
    blocks = blocks + [lax.ppermute(block, "mp", mates) for block in blocks]
    owners = owners + [owner ^ 1 for owner in owners]
    return jnp.concatenate(blocks, axis=0), jnp.stack(owners)


def relay_gather(rows, relay, home, other):
    count = lax.axis_size("mp")
    chips = count // 2
    both = ("section", "mp")
    me = lax.axis_index("mp")
    half = rows.shape[1] // 2

    def pairs(source, hops):
        return [
            (source * count + 2 * a + c, home * count + 2 * b + c)
            for a, b in hops
            for c in range(2)
        ]

    across = [(z, (z + 2) % chips) for z in range(chips)]
    ends = [(0, chips - 1), (chips - 1, 0)]
    up = [(z, z + 1) for z in range(chips - 1)]
    down = [(z + 1, z) for z in range(chips - 1)]
    mates = [(i, i ^ 1) for i in range(count)]
    near_half = lax.ppermute(rows[:, :half], both, pairs(home, across))
    wrapped = lax.ppermute(relay, both, pairs(other, ends))
    far_half = lax.ppermute(relay[:, half:], both, pairs(other, across))
    below = lax.ppermute(rows, both, pairs(home, up))
    above = lax.ppermute(rows, both, pairs(home, down))
    chip = me // 2
    below = jnp.where(chip == 0, wrapped, below)
    above = jnp.where(chip == chips - 1, wrapped, above)
    blocks = [rows, near_half, far_half, below, above]
    blocks = blocks + [lax.ppermute(block, "mp", mates) for block in blocks]
    owners = [me, (me - 4) % count, (me - 2) % count, (me + 2) % count]
    owners = owners + [owner ^ 1 for owner in owners]
    return jnp.concatenate(blocks, axis=1), jnp.stack(owners)


def row_positions(owners, length):
    local = jnp.arange(length, dtype=jnp.int32)
    if owners is None:
        return local
    rows_each = length // owners.shape[0]
    return (owners[:, None] * rows_each + local[None, :rows_each]).reshape(-1)


def move_rows(values, places):
    source = jnp.arange(values.shape[0], dtype=jnp.int32)
    pick = (source[:, None] == places[None, :]).astype(values.dtype)
    moved = jnp.dot(pick, values, preferred_element_type=jnp.float32)
    return moved.astype(values.dtype)


def attention_part(whole, owners, key_lengths, weight_qkv, weight_out):
    count = lax.axis_size("mp")
    requests = key_lengths.shape[0]
    length = whole.shape[0] // requests
    local_cols = weight_qkv.shape[2]
    heads = local_cols // HD
    parts = plane_products(whole, weight_qkv.transpose(1, 0, 2))
    if owners is None:
        parts = parts.reshape(3, count, requests, length // count, local_cols)
        parts = parts.transpose(0, 2, 1, 3, 4)
    parts = parts.reshape(3, requests, length, heads, HD)
    positions = row_positions(owners, length)
    valid = positions[None, :] < key_lengths[:, None]
    scores = jnp.einsum(
        "bqhe,bkhe->bhqk", parts[0], parts[1], preferred_element_type=jnp.float32
    ) * HD ** (-0.5)
    scores = jnp.where(valid[:, None, None, :], scores, -1000000000.0)
    probs = jax.nn.softmax(scores, axis=-1).astype(jnp.bfloat16)
    context = jnp.einsum("bhqk,bkhe->bqhe", probs, parts[2], preferred_element_type=jnp.float32)
    context = context.astype(jnp.bfloat16).reshape(requests * length, local_cols)
    each = length // count
    request = jnp.arange(requests, dtype=jnp.int32)[:, None]
    places = (positions // each)[None, :] * (requests * each) + request * each + positions % each
    context = move_rows(context, places.reshape(-1))
    partial_out = plane_products(context, weight_out[None], 1024)[0]
    return lax.psum_scatter(partial_out, "mp", scatter_dimension=0, tiled=True)


def forward_part(whole, weight_in, weight_down):
    inner = gated_products(whole, weight_in.transpose(1, 0, 2))
    partial_out = plane_products(inner, weight_down[None], 1024)[0]
    return lax.psum_scatter(partial_out, "mp", scatter_dimension=0, tiled=True)


def destinations(assign, per_group):
    count = assign.shape[0]
    order = jnp.arange(count, dtype=jnp.int32)
    same = assign[None, :] == assign[:, None]
    earlier = order[None, :] < order[:, None]
    slots = jnp.sum((same & earlier).astype(jnp.int32), axis=1)
    return assign * per_group + slots


def sum_over_mp(values):
    count = lax.axis_size("mp")
    step = 1
    while step < count:
        values = values + lax.ppermute(values, "mp", [(i, i ^ step) for i in range(count)])
        step *= 2
    return values


def per_device(
    tokens,
    lengths,
    assign,
    w_qkv,
    w_out,
    w_in,
    w_down,
    enc_gains,
    final_gain,
    w_memory,
    dec_input,
    dec_gain,
    w_query,
    w_cross_out,
):
    sections = lax.axis_size("section")
    section_id = lax.axis_index("section")
    req_count = lax.axis_size("req")
    req_id = lax.axis_index("req")
    mp_count = lax.axis_size("mp")
    local_rows, group_requests, width = tokens.shape
    full_length = local_rows * mp_count
    direct = mp_count // 2 <= 4
    relayed = mp_count // 2 == 4 and sections > 1

    groups = sections * req_count
    per_group = lengths.shape[0] // groups
    target = destinations(assign, per_group)
    mine = lax.dynamic_slice_in_dim(target, req_id * group_requests, group_requests)
    slot_ids = jnp.arange(groups * per_group, dtype=jnp.int32)
    group_id = section_id * req_count + req_id
    picker_all = (target[None, :] == slot_ids[:, None]).astype(jnp.float32)
    picker = lax.dynamic_slice_in_dim(picker_all, group_id * per_group, per_group, 0)
    query_rows = jnp.dot(picker, dec_input.astype(jnp.float32), precision=lax.Precision.HIGHEST)
    query_lengths = jnp.sum(jnp.where(picker > 0.5, lengths[None, :], 0), axis=1)
    dec_normed = rms_norm(query_rows, dec_gain).astype(jnp.bfloat16)
    local_cols = w_query.shape[1]
    local_heads = local_cols // HD
    query = (
        jnp.dot(dec_normed, w_query, preferred_element_type=jnp.float32)
        .astype(jnp.bfloat16)
        .reshape(per_group, local_heads, HD)
    )

    key_lengths = lax.dynamic_slice_in_dim(lengths, req_id * group_requests, group_requests)
    gain = enc_gains[0, 0]
    flat = (group_requests * local_rows, width)

    def norm_rows(values, by):
        return rms_norm(values.astype(jnp.float32), by).astype(jnp.bfloat16)

    hidden = tokens.transpose(1, 0, 2)
    for layer in range(sections):
        other = layer - 1
        relay_here = relayed and layer > 0
        if relay_here:
            relay = norm_rows(hidden, lax.ppermute(gain, "section", [(layer, other)]))
        if layer > 0:
            hidden = lax.ppermute(hidden, "section", [(layer - 1, layer)])
        normed = norm_rows(hidden, gain)
        if relay_here:
            whole, owners = relay_gather(normed, relay, layer, other)
            whole = whole.reshape(-1, width)
        else:
            whole, owners = lax.all_gather(normed.reshape(flat), "mp", axis=0, tiled=True), None
        part = attention_part(whole, owners, key_lengths, w_qkv[0], w_out[0])
        stream = hidden.astype(jnp.float32) + part.astype(jnp.float32).reshape(hidden.shape)
        normed = norm_rows(stream, enc_gains[0, 1]).reshape(flat)
        part = forward_part(
            lax.all_gather(normed, "mp", axis=0, tiled=True), w_in[0], w_down[0]
        )
        if layer == sections - 1:
            memory_planes = w_memory.transpose(1, 0, 2)
            part, memory_planes = lax.optimization_barrier((part, memory_planes))
        stream = stream + part.astype(jnp.float32).reshape(stream.shape)
        hidden = stream.astype(jnp.bfloat16)

    last = rms_norm(hidden.astype(jnp.float32), final_gain).astype(jnp.bfloat16)
    normed = [last[j] for j in range(group_requests)]
    chosen = mine[None, :] == slot_ids[:, None]
    outgoing = sum(
        jnp.where(chosen[:, r, None, None], normed[r][None], jnp.bfloat16(0))
        for r in range(group_requests)
    )
    incoming = lax.all_to_all(outgoing, ("section", "req"), split_axis=0, concat_axis=0, tiled=True)
    incoming = incoming.reshape(sections, req_count, per_group, local_rows, width)[sections - 1]
    received = incoming[0]
    for source in range(1, req_count):
        received = received + incoming[source]
    gathered, owners = gather_rows(
        received.transpose(1, 0, 2).reshape(local_rows * per_group, width), direct
    )
    columns = plane_products(gathered, memory_planes)
    columns = columns.transpose(1, 0, 2).reshape(full_length * per_group, 2 * local_cols)
    if owners is not None:
        block = local_rows * per_group
        inside = jnp.arange(block, dtype=jnp.int32)
        columns = move_rows(columns, (owners[:, None] * block + inside[None, :]).reshape(-1))
    columns = columns.reshape(full_length, per_group, 2, local_cols)
    memory_kv = columns.transpose(1, 0, 2, 3)
    columns = [columns[:, :, 0], columns[:, :, 1]]
    cross_keys = columns[0].reshape(full_length, per_group, local_heads, HD)
    cross_values = columns[1].reshape(full_length, per_group, local_heads, HD)
    positions = jnp.arange(full_length, dtype=jnp.int32)
    scores = jnp.einsum(
        "ohe,lohe->ohl", query, cross_keys, preferred_element_type=jnp.float32
    ) * HD ** (-0.5)
    scores = jnp.where(
        positions[None, None, :] < query_lengths[:, None, None], scores, -1000000000.0
    )
    weights = jax.nn.softmax(scores, axis=-1).astype(jnp.bfloat16)
    context = jnp.einsum(
        "ohl,lohe->ohe", weights, cross_values, preferred_element_type=jnp.float32
    ).astype(jnp.bfloat16)
    partial_out = jnp.dot(
        context.reshape(per_group, local_cols), w_cross_out, preferred_element_type=jnp.float32
    )
    total_out = sum_over_mp(partial_out)
    dec_output = (query_rows + total_out).astype(jnp.bfloat16)
    return (memory_kv, dec_output)


def solution(mesh):
    return jax.shard_map(
        per_device,
        mesh=mesh,
        in_specs=(
            P("mp", "req", None),
            P(),
            P(),
            P("section", None, None, "mp"),
            P("section", "mp", None),
            P("section", None, None, "mp"),
            P("section", "mp", None),
            P("section", None, None),
            P(),
            P(None, None, "mp"),
            P(),
            P(),
            P(None, "mp"),
            P("mp", None),
        ),
        out_specs=(P(("section", "req"), None, None, "mp"), P(("section", "req"), None)),
        check_vma=False,
    )
```
